32 devices in a mesh: gx: 2 (over x), gy: 4 (over y, core), gz: 4 (over z).
Axes of the slice: x: 2, y: 2, z: 4, core: 2. Of those that a mesh axis runs over, the one named last changes fastest.
Arguments:
- grains: float32 [12, 32, 32, 512], P(None, 'gz', 'gx', 'gy'), may hold values from 0 to 0.6
- solute: float32 [32, 32, 512], P('gz', 'gx', 'gy'), may hold values from 0 to 0.6
- thermal: float32 [4, 2, 4, 20, 4096], P('gz', 'gx', 'gy'), may hold values from 0.5 to 1.5
- block_slot: int32 [4, 2, 4, 20], P('gz', 'gx', 'gy'), may hold values from -1 to 19, as said below
- block_owner: int32 [4, 2, 4, 20], P('gz', 'gx', 'gy'), may hold values from -1 to 3, as said below
- block_offset: int32 [4, 2, 4, 3, 20], P('gz', 'gx', 'gy'), may hold values from -31 to 128, as said below
Outputs:
- grains_out: float32 [12, 32, 32, 512], P(None, 'gz', 'gx', 'gy')
- solute_out: float32 [32, 32, 512], P('gz', 'gx', 'gy')
- temperature: float32 [32, 32, 512], P('gz', 'gx', 'gy')
The draws below stay inside these ranges and needn't reach their ends.
Inputs may be any that keep to these rules, and one draw needn't show every extreme that they name: `block_slot`: -1 exactly where block_owner is -1; the live entries of all tiles name distinct pairs (owner, slot) within a column. `block_owner`: -1 marks an empty entry. No owner serves more than 5 live entries of one tile; in every draw, in each column, some owner serves 5 entries of every tile of that column; and in every draw some tile of the box has all 20 entries live. `block_offset`: 0 for empty entries. Along each dimension the live starts of a tile differ by multiples of 32, and the hats of a tile's live blocks sum to one at each of its cells.
All inputs are finite; a program needn't handle non-finite values.
Results may differ from the reference program's by a relative error of at most 0.0003.
Values sent between devices are 32-bit elements; how exact they have to be, the bound alone decides.
No kernel may reach another device: no remote copies, remote signals or barrier semaphores. Data moves between devices by JAX's collectives and lax.ppermute only.
A program may use at most 64 MiB of HBM per device.

```python
import jax
import jax.numpy as jnp
from jax import lax

GRAINS = 12
BLOCK = 16
STEPS = 3
CZ = 8
CX = 16
CY = 128
SPAN = 32
KZ = 2
KX = 2
KY = 5
MAXB = 20
CAP = 5
TILES_Z = 4
TILES_X = 2
TILES_Y = 4
SLOTS = 20
NZ = 32
NX = 32
NY = 512


def axis_blocks(phases, length, reach_count):
    steps_index = jnp.arange(reach_count, dtype=jnp.int32)
    usable = steps_index[None, None, None, :] <= (length + phases[..., None]) // SPAN
    anchor = SPAN * steps_index[None, None, None, :] - phases[..., None]
    return (usable, anchor)


def layout(key):
    folded = jax.random.fold_in(key, 4242)
    subkeys = jax.random.split(folded, 5)
    tile_grid = (TILES_Z, TILES_X, TILES_Y)
    tiles = TILES_Z * TILES_X * TILES_Y
    phases = jax.random.randint(subkeys[0], tile_grid + (3,), 0, SPAN)
    chosen = jax.random.randint(subkeys[1], (), 0, tiles)
    numbered = jnp.arange(tiles, dtype=jnp.int32).reshape(tile_grid)
    phases = jnp.where((numbered == chosen)[..., None], SPAN - 1, phases)
    usable_z, anchor_z = axis_blocks(phases[..., 0], CZ, KZ)
    usable_x, anchor_x = axis_blocks(phases[..., 1], CX, KX)
    usable_y, anchor_y = axis_blocks(phases[..., 2], CY, KY)
    full_shape = tile_grid + (KZ, KX, KY)
    usable = usable_z[..., :, None, None] & usable_x[..., None, :, None] & usable_y[..., None, None, :]
    usable = usable.reshape(tile_grid + (MAXB,))
    corner_z = jnp.broadcast_to(anchor_z[..., :, None, None], full_shape).reshape(tile_grid + (MAXB,))
    corner_x = jnp.broadcast_to(anchor_x[..., None, :, None], full_shape).reshape(tile_grid + (MAXB,))
    corner_y = jnp.broadcast_to(anchor_y[..., None, None, :], full_shape).reshape(tile_grid + (MAXB,))
    corners = jnp.stack([corner_z, corner_x, corner_y], axis=3)
    scores = jax.random.randint(subkeys[2], tile_grid + (MAXB,), 0, 1 << 20) * MAXB + jnp.arange(MAXB, dtype=jnp.int32)
    shuffle = jnp.argsort(scores, axis=-1)
    usable = jnp.take_along_axis(usable, shuffle, axis=-1)
    corners = jnp.take_along_axis(corners, jnp.broadcast_to(shuffle[..., None, :], corners.shape), axis=-1)
    counted = jnp.maximum(jnp.cumsum(usable.astype(jnp.int32), axis=-1) - 1, 0)
    ranked = jax.random.randint(subkeys[3], (TILES_X, TILES_Y, TILES_Z), 0, 1 << 20) * TILES_Z + jnp.arange(TILES_Z, dtype=jnp.int32)
    column_order = jnp.argsort(ranked, axis=-1).astype(jnp.int32)
    holder_rank = counted // CAP
    z_index = jnp.arange(TILES_Z, dtype=jnp.int32)[:, None, None, None]
    x_index = jnp.arange(TILES_X, dtype=jnp.int32)[None, :, None, None]
    y_index = jnp.arange(TILES_Y, dtype=jnp.int32)[None, None, :, None]
    holders = column_order[x_index, y_index, holder_rank]
    placed = jax.random.randint(subkeys[4], (TILES_Z, TILES_X, TILES_Y, SLOTS), 0, 1 << 20) * SLOTS + jnp.arange(SLOTS, dtype=jnp.int32)
    slot_order = jnp.argsort(placed, axis=-1).astype(jnp.int32)
    seat_index = z_index * CAP + counted % CAP
    slot_ids = slot_order[holders, x_index, y_index, seat_index]
    holders = jnp.where(usable, holders, -1).astype(jnp.int32)
    slot_ids = jnp.where(usable, slot_ids, -1).astype(jnp.int32)
    corners = jnp.where(usable[..., None, :], corners, 0).astype(jnp.int32)
    return (slot_ids, holders, corners)


def draw_block_slot(key, part):
    return layout(key)[0]


def draw_block_owner(key, part):
    return layout(key)[1]


def draw_block_offset(key, part):
    return layout(key)[2]


def levels(key, shape, cuts, smallest, high):
    gain = 1.0
    for position, parts in cuts:
        draws = jax.random.uniform(jax.random.fold_in(jax.random.fold_in(key, 6), position), (parts,), jnp.float32, smallest / len(cuts), high / len(cuts))
        gain = gain * jnp.repeat(jnp.exp(draws), shape[position] // parts).reshape((-1,) + (1,) * (len(shape) - 1 - position))
    return gain


def setup_inputs(seed: int = 0) -> dict:
    arg_keys = jax.random.split(jax.random.key(seed), 7)
    grains = jnp.clip(0.6 * jax.random.uniform(arg_keys[0], (GRAINS, NZ, NX, NY), jnp.float32) ** levels(arg_keys[0], (GRAINS, NZ, NX, NY), ((1, 4), (2, 2), (3, 4)), -0.2, 0.2), 0.0, 0.6)
    solute = jnp.clip(0.6 * jax.random.uniform(arg_keys[1], (NZ, NX, NY), jnp.float32) ** levels(arg_keys[1], (NZ, NX, NY), ((0, 4), (1, 2), (2, 4)), -0.2, 0.2), 0.0, 0.6)
    thermal = jnp.clip(0.5 + 1.0 * jax.random.uniform(arg_keys[2], (TILES_Z, TILES_X, TILES_Y, SLOTS, BLOCK ** 3), jnp.float32) ** levels(arg_keys[2], (TILES_Z, TILES_X, TILES_Y, SLOTS, BLOCK ** 3), ((0, 4), (1, 2), (2, 4)), -0.2, 0.2), 0.5, 1.5)
    block_slot = draw_block_slot(jax.random.fold_in(arg_keys[6], 71), 0)
    block_owner = draw_block_owner(jax.random.fold_in(arg_keys[6], 71), 0)
    block_offset = draw_block_offset(jax.random.fold_in(arg_keys[6], 71), 0)
    return dict(grains=grains, solute=solute, thermal=thermal, block_slot=block_slot, block_owner=block_owner, block_offset=block_offset)


step_rate = 0.1
stiffness = 1.6
cross_energy = 0.25
drive_scale = 2.0
liquidus_slope = 0.5
rejection = 0.5
diffusion_rate = 0.15


def hat_weights(starts, cell_count):
    positions = jnp.arange(cell_count, dtype=jnp.float32)
    node_sites = 2.0 * jnp.arange(BLOCK, dtype=jnp.float32)
    distance = positions[None, :, None] - starts.astype(jnp.float32)[:, None, None] - node_sites[None, None, :]
    return jnp.maximum(0.0, 1.0 - jnp.abs(distance) / 2.0)


def project(blocks, starts, live_entry, layers, breadth, length):
    entries = blocks.shape[0]
    cubes = blocks.reshape(entries, BLOCK, BLOCK, BLOCK)
    weight_z = hat_weights(starts[0], layers) * live_entry.astype(jnp.float32)[:, None, None]
    weight_x = hat_weights(starts[1], breadth)
    weight_y = hat_weights(starts[2], length)
    along_y = jnp.einsum("epqr,eyr->epqy", cubes, weight_y, precision=lax.Precision.HIGHEST)
    along_x = jnp.einsum("exq,epqy->epxy", weight_x, along_y, precision=lax.Precision.HIGHEST)
    return weight_z, along_x


def laplace(padded):
    middle = padded[..., 1:-1, 1:-1, 1:-1]
    return (padded[..., 2:, 1:-1, 1:-1] + padded[..., :-2, 1:-1, 1:-1]
            + padded[..., 1:-1, 2:, 1:-1] + padded[..., 1:-1, :-2, 1:-1]
            + padded[..., 1:-1, 1:-1, 2:] + padded[..., 1:-1, 1:-1, :-2] - 6.0 * middle)


def advance(padded, heat_field):
    orders = padded[:-1]
    concentration = padded[-1]
    squares = jnp.sum(orders * orders, axis=0)
    bending = laplace(orders)
    diffusion_term = laplace(concentration - rejection * squares)
    central = orders[:, 1:-1, 1:-1, 1:-1]
    central_sum = squares[1:-1, 1:-1, 1:-1]
    central_solute = concentration[1:-1, 1:-1, 1:-1]
    undercool = drive_scale * (1.0 - heat_field - liquidus_slope * central_solute)
    double_well = 2.0 * central * (1.0 - central) * (1.0 - 2.0 * central)
    contact_term = 4.0 * cross_energy * central * (central_sum - central * central)
    growth_term = 30.0 * central * central * (1.0 - central) * (1.0 - central) * undercool
    new_orders = central + step_rate * (stiffness * bending - double_well - contact_term + growth_term)
    new_solute = central_solute + diffusion_rate * diffusion_term
    return jnp.concatenate([new_orders, new_solute[None]], axis=0)


def tile_heat(flat_tile, thermal, block_slot, block_owner, block_offset):
    tile_layer = flat_tile // (TILES_X * TILES_Y)
    tile_row = (flat_tile // TILES_Y) % TILES_X
    tile_col = flat_tile % TILES_Y
    slot_ids = block_slot[tile_layer, tile_row, tile_col]
    holders = block_owner[tile_layer, tile_row, tile_col]
    starts = block_offset[tile_layer, tile_row, tile_col]
    live_entry = holders >= 0
    blocks = thermal[jnp.clip(holders, 0, TILES_Z - 1), tile_row, tile_col, jnp.clip(slot_ids, 0, SLOTS - 1)]
    weight_z, along_x = project(blocks, starts, live_entry, CZ, CX, CY)
    return jnp.einsum("ezp,epxy->zxy", weight_z, along_x, precision=lax.Precision.HIGHEST)


def reference(grains, solute, thermal, block_slot, block_owner, block_offset):
    tiles = jnp.arange(TILES_Z * TILES_X * TILES_Y, dtype=jnp.int32)
    pieces = lax.map(lambda flat_tile: tile_heat(flat_tile, thermal, block_slot, block_owner, block_offset), tiles)
    pieces = pieces.reshape(TILES_Z, TILES_X, TILES_Y, CZ, CX, CY)
    heat_field = jnp.transpose(pieces, (0, 3, 1, 4, 2, 5)).reshape(NZ, NX, NY)
    fields = jnp.concatenate([grains, solute[None]], axis=0)
    for repeat in range(STEPS):
        padded = jnp.pad(fields, ((0, 0), (0, 0), (1, 1), (1, 1)), mode="wrap")
        padded = jnp.pad(padded, ((0, 0), (1, 1), (0, 0), (0, 0)), mode="symmetric")
        fields = advance(padded, heat_field)
    return fields[:-1], fields[-1], heat_field
```

```python
import functools

import jax
import jax.numpy as jnp
from jax import lax
from jax.experimental import pallas as pl
from jax.experimental.pallas import tpu as pltpu
from jax.sharding import PartitionSpec as P

NODES = 16
STEPS = 3
LANES = 128
ROWS = 8
FAR = 4096

VMEM = pl.BlockSpec(memory_space=pltpu.VMEM)
SMEM = pl.BlockSpec(memory_space=pltpu.SMEM)


def half_up(start):
    return (start + (start & 1)) >> 1


def route_kernel(ring, capacity, slot_ref, owner_ref, start_ref, *rest):
    lists, parity, picks = rest[:ring], rest[ring], rest[ring + 1]
    entries = slot_ref.shape[-1]
    me = lax.axis_index("gz")
    owners = [owner_ref[0, 0, 0, e] for e in range(entries)]
    for axis in range(2):
        odd = jnp.int32(0)
        for e in range(entries):
            odd = odd | jnp.where(owners[e] >= 0, start_ref[0, 0, 0, axis, e] & 1, 0)
        parity[axis] = odd
    for distance in range(ring):
        target = lax.rem(me + distance, ring)
        found = jnp.int32(0)
        for e in range(entries):
            picks[found] = e
            found = found + (owners[e] == target).astype(jnp.int32)
        for c in range(capacity):
            held = c < found
            e = jnp.where(held, picks[c], 0)
            lists[distance][4 * c] = jnp.maximum(slot_ref[0, 0, 0, e], 0)
            for axis in range(3):
                lists[distance][4 * c + 1 + axis] = jnp.where(held, start_ref[0, 0, 0, axis, e], FAR)


def project_kernel(ring, capacity, columns, *refs):
    lists, thermal, outs = refs[:ring], refs[ring], refs[ring + 1 :]
    node_x = lax.broadcasted_iota(jnp.int32, (2 * ROWS, NODES * NODES), 1) // NODES
    plane = lax.broadcasted_iota(jnp.int32, (ROWS, NODES * NODES), 0)
    cell_y = lax.broadcasted_iota(jnp.int32, (NODES, LANES), 1)
    node_y = 2 * lax.broadcasted_iota(jnp.int32, (NODES, LANES), 0)
    for distance in range(ring):
        total = None
        for c in range(capacity):
            slot, z, x, y = (lists[distance][4 * c + i] for i in range(4))
            rise = half_up(z)
            planes = pltpu.roll(thermal[slot], rise & (NODES - 1), 0)[:ROWS]
            planes = jnp.where((plane >= rise) & (plane < rise + NODES), planes, 0.0)
            coarse = planes.astype(jnp.bfloat16).astype(jnp.float32)
            pair = jnp.concatenate([coarse, planes - coarse], axis=0).astype(jnp.bfloat16)
            shift = half_up(x)
            spread = jnp.concatenate(
                [pair * (node_x == j - shift).astype(jnp.float32).astype(jnp.bfloat16) for j in range(columns)],
                axis=0,
            )
            distance_y = (cell_y - y - node_y).astype(jnp.float32)
            hat = jnp.maximum(0.0, 1.0 - 0.5 * jnp.abs(distance_y)).astype(jnp.bfloat16)
            part = jnp.dot(spread, jnp.concatenate([hat] * NODES, axis=0), preferred_element_type=jnp.float32)
            total = part if total is None else total + part
        total = total.reshape(columns, 2, ROWS, LANES)
        outs[distance][...] = total[:, 0] + total[:, 1]


class Faces:
    def __init__(self, count, layers, breadth, x_low, x_high, y_out, z_low, z_high):
        self.count, self.layers, self.breadth = count, layers, breadth
        self.halves = breadth // ROWS
        self.width = 2 * layers * self.halves
        self.per = LANES // self.width
        self.groups = -(-count // self.per)
        self.x_low, self.x_high, self.y_out = x_low, x_high, y_out
        self.z_low, self.z_high = z_low, z_high

    def start(self):
        return tuple(jnp.zeros((ROWS, LANES), jnp.float32) for _ in range(self.groups))

    def lane(self, f, z, half):
        return (f % self.per) * self.width + 2 * (z * self.halves + half)

    def add(self, carry, f, z, cells, lanes):
        carry = list(carry)
        self.x_low[f, pl.ds(z, 1), :] = cells[:1]
        self.x_high[f, pl.ds(z, 1), :] = cells[-1:]
        group = f // self.per
        for half in range(self.halves):
            k = self.lane(f, z, half)
            turned = pltpu.roll(cells[half * ROWS : (half + 1) * ROWS], k + 1, 1)
            carry[group] = jnp.where((lanes >> 1) == (k >> 1), turned, carry[group])
        return tuple(carry)

    def finish(self, carry, fields, extra):
        for group in range(self.groups):
            self.y_out[group] = carry[group]
        for f in range(self.count - 1):
            self.z_low[f] = fields[f, 0]
            self.z_high[f] = fields[f, self.layers - 1]
        self.z_low[self.count - 1] = extra[0]
        self.z_high[self.count - 1] = extra[self.layers - 1]


def split_x(refs, together):
    if together:
        return (refs[0].at[0], refs[0].at[1]), refs[1:]
    return (refs[0], refs[1]), refs[2:]


def pack_kernel(together, grains, solute, mixed, *rest):
    (x_low, x_high), (y_out, z_low, z_high) = split_x(rest, together)
    orders, layers, breadth, _ = grains.shape
    faces = Faces(orders + 1, layers, breadth, x_low, x_high, y_out, z_low, z_high)
    lanes = lax.broadcasted_iota(jnp.int32, (ROWS, LANES), 1)

    def layer(z, carry):
        squares = None
        for f in range(orders):
            cells = grains[f, z]
            squares = cells * cells if squares is None else squares + cells * cells
            carry = faces.add(carry, f, z, cells, lanes)
        value = solute[z] - 0.5 * squares
        mixed[z] = value
        return faces.add(carry, orders, z, value, lanes)

    faces.finish(lax.fori_loop(0, layers, layer, faces.start()), grains, mixed)


def step_kernel(first, last, together, ring, columns, *refs):
    refs = list(refs)
    take = lambda n: [refs.pop(0) for _ in range(n)]
    fields, solute, mixed = take(3)
    if first:
        parts = take(ring)
        (parity,) = take(1)
    else:
        (heat,) = take(1)
    if together:
        (arrived,) = take(1)
        x_low, x_high = arrived.at[1], arrived.at[0]
    else:
        x_low, x_high = take(2)
    y_low, y_high, z_low, z_high = take(4)
    fields_out, solute_out = take(2)
    if first:
        (heat,) = take(1)
    orders, layers, breadth, _ = fields.shape
    count = orders + 1
    if last:
        wide, turned = take(2)
        faces = Faces(count, layers, breadth, None, None, None, None, None)
    else:
        (mixed_out,) = take(1)
        (out_low, out_high), refs = split_x(refs, together)
        out_y, out_z_low, out_z_high, wide, turned = refs
        faces = Faces(count, layers, breadth, out_low, out_high, out_y, out_z_low, out_z_high)
    lanes = lax.broadcasted_iota(jnp.int32, (ROWS, LANES), 1)

    place = lax.axis_index("gz")
    at_bottom = place == 0
    at_top = place == ring - 1
    for f in range(count):
        source = fields.at[f] if f < orders else mixed
        wide[f, 1 : layers + 1, ROWS : ROWS + breadth, :] = source[...]
        wide[f, 0, ROWS : ROWS + breadth, :] = jnp.where(at_bottom, source[0], z_low[f])
        wide[f, layers + 1, ROWS : ROWS + breadth, :] = jnp.where(at_top, source[layers - 1], z_high[f])
        wide[f, 1 : layers + 1, ROWS - 1, :] = x_low[f]
        wide[f, 1 : layers + 1, ROWS + breadth, :] = x_high[f]
    for group in range(faces.groups):
        turned[group] = jnp.where(
            (lanes & 1) == 1, pltpu.roll(y_low[group], 1, 1), pltpu.roll(y_high[group], LANES - 1, 1)
        )

    if first:
        lattice = parts[0][...]
        for part in parts[1:]:
            lattice = lattice + part[...]
        coarse = lattice.astype(jnp.bfloat16).astype(jnp.float32)
        pair = jnp.concatenate([coarse, lattice - coarse], axis=1)
        pair = pair.reshape(columns * 2 * ROWS, LANES).astype(jnp.bfloat16)
        shape = (layers * breadth, columns * 2 * ROWS)
        cell = lax.broadcasted_iota(jnp.int32, shape, 0)
        node = lax.broadcasted_iota(jnp.int32, shape, 1)

        def hat(position, index, odd):
            gap = (position + odd - 2 * index).astype(jnp.float32)
            return jnp.maximum(0.0, 1.0 - 0.5 * jnp.abs(gap))

        weight = hat(cell // breadth, node % ROWS, parity[0]) * hat(cell % breadth, node // (2 * ROWS), parity[1])
        warm = jnp.dot(weight.astype(jnp.bfloat16), pair, preferred_element_type=jnp.float32)
        heat[...] = warm.reshape(layers, breadth, LANES)

    def around(f, z, cells):
        span = slice(ROWS, ROWS + breadth)
        total = wide[f, z, span, :] + wide[f, z + 2, span, :]
        total = total + wide[f, z + 1, ROWS - 1 : ROWS - 1 + breadth, :]
        total = total + wide[f, z + 1, ROWS + 1 : ROWS + 1 + breadth, :]
        sides = []
        for half in range(faces.halves):
            piece = cells[half * ROWS : (half + 1) * ROWS]
            k = faces.lane(f, z, half)
            beyond = pltpu.roll(turned[f // faces.per], LANES - 1 - k, 1)
            below = jnp.where(lanes == 0, beyond, pltpu.roll(piece, 1, 1))
            above = jnp.where(lanes == LANES - 1, beyond, pltpu.roll(piece, LANES - 1, 1))
            sides.append(below + above)
        return total + jnp.concatenate(sides, axis=0)

    def layer(z, carry):
        squares = None
        for f in range(orders):
            cells = fields[f, z]
            squares = cells * cells if squares is None else squares + cells * cells
        here = solute[z]
        pull = 0.04 - 0.1 * squares
        drive = 6.0 * (1.0 - heat[z] - 0.5 * here)
        level = mixed[z]
        fresh = here + 0.15 * (around(orders, z, level) - 6.0 * level)
        solute_out[z] = fresh
        squares = None
        for f in range(orders):
            cells = fields[f, z]
            well = cells * (1.0 - cells)
            value = (
                0.16 * around(f, z, cells)
                + cells * (pull + 0.1 * (cells * cells))
                + well * (drive * well + (0.4 * cells - 0.2))
            )
            fields_out[f, z] = value
            if not last:
                squares = value * value if squares is None else squares + value * value
                carry = faces.add(carry, f, z, value, lanes)
        if last:
            return carry
        value = fresh - 0.5 * squares
        mixed_out[z] = value
        return faces.add(carry, orders, z, value, lanes)

    carry = lax.fori_loop(0, layers, layer, () if last else faces.start())
    if not last:
        faces.finish(carry, fields_out, mixed_out)


def shape_of(*dims, dtype=jnp.float32):
    return jax.ShapeDtypeStruct(dims, dtype)


def cost(flops, moved):
    return pl.CostEstimate(flops=flops, bytes_accessed=moved, transcendentals=0)


def around_ring(axis, distance):
    count = lax.axis_size(axis)
    return [(i, (i + distance) % count) for i in range(count)]


def body(grains, solute, thermal, block_slot, block_owner, block_offset):
    ring = lax.axis_size("gz")
    across = lax.axis_size("gx")
    together = across == 2
    orders, layers, breadth, length = grains.shape
    slots = thermal.shape[3]
    capacity = slots // ring
    columns = breadth // 2 + 1
    count = orders + 1
    assert length == LANES and breadth % ROWS == 0 and layers // 2 + 1 <= ROWS

    routed = pl.pallas_call(
        functools.partial(route_kernel, ring, capacity),
        out_shape=[shape_of(4 * capacity, dtype=jnp.int32)] * ring + [shape_of(2, dtype=jnp.int32)],
        in_specs=[SMEM] * 3,
        out_specs=[SMEM] * (ring + 1),
        scratch_shapes=[pltpu.SMEM((block_slot.shape[-1] + 1,), jnp.int32)],
        name="route",
    )(block_slot, block_owner, block_offset)
    asked, parity = routed[:ring], routed[ring]
    asked = [asked[0]] + [lax.ppermute(asked[d], "gz", around_ring("gz", d)) for d in range(1, ring)]

    sizes = Faces(count, layers, breadth, None, None, None, None, None)
    face_x = [shape_of(2, count, layers, length)] if together else [shape_of(count, layers, length)] * 2
    face_shapes = face_x + [shape_of(sizes.groups, ROWS, LANES)] + [shape_of(count, breadth, length)] * 2
    tile = shape_of(layers, breadth, length)

    packed = pl.pallas_call(
        functools.partial(pack_kernel, together),
        out_shape=[tile] + face_shapes,
        in_specs=[VMEM] * 2,
        out_specs=[VMEM] * (1 + len(face_shapes)),
        cost_estimate=cost(4_000_000, 2_000_000),
        name="pack",
    )(grains, solute)

    def exchange(faces):
        if together:
            moved = [lax.ppermute(faces[0], "gx", around_ring("gx", 1))]
        else:
            moved = [
                lax.ppermute(faces[1], "gx", around_ring("gx", 1)),
                lax.ppermute(faces[0], "gx", around_ring("gx", -1)),
            ]
        y_out, z_low, z_high = faces[-3:]
        up = [(i, i + 1) for i in range(ring - 1)]
        down = [(i + 1, i) for i in range(ring - 1)]
        return moved + [
            lax.ppermute(y_out, "gy", around_ring("gy", 1)),
            lax.ppermute(y_out, "gy", around_ring("gy", -1)),
            lax.ppermute(z_high, "gz", up),
            lax.ppermute(z_low, "gz", down),
        ]

    mixed, faces = packed[0], packed[1:]
    arrived = exchange(faces)

    nodes = thermal.reshape(slots, NODES, NODES * NODES)
    lattice = shape_of(columns, ROWS, length)
    parts = pl.pallas_call(
        functools.partial(project_kernel, ring, capacity, columns),
        out_shape=[lattice] * ring,
        in_specs=[SMEM] * ring + [VMEM],
        out_specs=[VMEM] * ring,
        cost_estimate=cost(4_000_000, 1_000_000),
        name="project",
    )(*asked, nodes)
    parts = [parts[0]] + [lax.ppermute(parts[d], "gz", around_ring("gz", -d)) for d in range(1, ring)]

    fields = grains
    heat = None
    for repeat in range(STEPS):
        first, last = repeat == 0, repeat == STEPS - 1
        extra = list(parts) + [parity] if first else [heat]
        extra_specs = [VMEM] * ring + [SMEM] if first else [VMEM]
        out_shape = [shape_of(*grains.shape), tile]
        if first:
            out_shape = out_shape + [tile]
        if not last:
            out_shape = out_shape + [tile] + face_shapes
        outs = pl.pallas_call(
            functools.partial(step_kernel, first, last, together, ring, columns),
            out_shape=out_shape,
            in_specs=[VMEM] * 3 + extra_specs + [VMEM] * len(arrived),
            out_specs=[VMEM] * len(out_shape),
            scratch_shapes=[
                pltpu.VMEM((count, layers + 2, breadth + 2 * ROWS, LANES), jnp.float32),
                pltpu.VMEM((sizes.groups, ROWS, LANES), jnp.float32),
            ],
            cost_estimate=cost(8_000_000, 3_000_000),
            name=f"step{repeat}",
        )(fields, solute, mixed, *extra, *arrived)
        fields, solute = outs[:2]
        outs = list(outs[2:])
        if first:
            heat = outs.pop(0)
        if not last:
            mixed, faces = outs[0], outs[1:]
            arrived = exchange(faces)
    return (fields, solute, heat)


def solution(mesh):
    in_specs = (
        P(None, "gz", "gx", "gy"),
        P("gz", "gx", "gy"),
        P("gz", "gx", "gy", None, None),
        P("gz", "gx", "gy", None),
        P("gz", "gx", "gy", None),
        P("gz", "gx", "gy", None, None),
    )
    out_specs = (P(None, "gz", "gx", "gy"), P("gz", "gx", "gy"), P("gz", "gx", "gy"))
    return jax.shard_map(body, mesh=mesh, in_specs=in_specs, out_specs=out_specs, check_vma=False)
```

```python
import functools

import jax
import jax.numpy as jnp
from jax import lax
from jax.experimental import pallas as pl
from jax.experimental.pallas import tpu as pltpu
from jax.sharding import PartitionSpec as P

NODES = 16
STEPS = 3
LANES = 128
ROWS = 8
FAR = 4096

VMEM = pl.BlockSpec(memory_space=pltpu.VMEM)
SMEM = pl.BlockSpec(memory_space=pltpu.SMEM)

PARAMS = pltpu.CompilerParams(vmem_limit_bytes=12 * 1024 * 1024)


def half_up(start):
    return (start + (start & 1)) >> 1


def route_kernel(ring, capacity, slot_ref, owner_ref, start_ref, *rest):
    lists, parity, picks = rest[:ring], rest[ring], rest[ring + 1]
    entries = slot_ref.shape[-1]
    me = lax.axis_index("gz")
    owners = [owner_ref[0, 0, 0, e] for e in range(entries)]
    for axis in range(2):
        odd = jnp.int32(0)
        for e in range(entries):
            odd = odd | jnp.where(owners[e] >= 0, start_ref[axis, 0, e] & 1, 0)
        parity[axis] = odd
    for distance in range(ring):
        target = lax.rem(me + distance, ring)
        found = jnp.int32(0)
        for e in range(entries):
            picks[found] = e
            found = found + (owners[e] == target).astype(jnp.int32)
        for c in range(capacity):
            held = c < found
            e = jnp.where(held, picks[c], 0)
            lists[distance][4 * c] = jnp.maximum(slot_ref[0, 0, 0, e], 0)
            for axis in range(3):
                lists[distance][4 * c + 1 + axis] = jnp.where(held, start_ref[axis, 0, e], FAR)


def project_kernel(ring, capacity, columns, *refs):
    lists, thermal, outs = refs[:ring], refs[ring], refs[ring + 1 :]
    node_x = lax.broadcasted_iota(jnp.int32, (2 * ROWS, NODES * NODES), 1) // NODES
    plane = lax.broadcasted_iota(jnp.int32, (ROWS, NODES * NODES), 0)
    cell_y = lax.broadcasted_iota(jnp.int32, (NODES, LANES), 1)
    node_y = 2 * lax.broadcasted_iota(jnp.int32, (NODES, LANES), 0)
    for distance in range(ring):
        total = None
        for c in range(capacity):
            slot, z, x, y = (lists[distance][4 * c + i] for i in range(4))
            rise = half_up(z)
            planes = pltpu.roll(thermal[slot], rise & (NODES - 1), 0)[:ROWS]
            planes = jnp.where((plane >= rise) & (plane < rise + NODES), planes, 0.0)
            coarse = planes.astype(jnp.bfloat16).astype(jnp.float32)
            pair = jnp.concatenate([coarse, planes - coarse], axis=0).astype(jnp.bfloat16)
            shift = half_up(x)
            spread = jnp.concatenate(
                [pair * (node_x == j - shift).astype(jnp.float32).astype(jnp.bfloat16) for j in range(columns)],
                axis=0,
            )
            distance_y = (cell_y - y - node_y).astype(jnp.float32)
            hat = jnp.maximum(0.0, 1.0 - 0.5 * jnp.abs(distance_y)).astype(jnp.bfloat16)
            part = jnp.dot(spread, jnp.concatenate([hat] * NODES, axis=0), preferred_element_type=jnp.float32)
            total = part if total is None else total + part
        total = total.reshape(columns, 2, ROWS, LANES)
        outs[distance][...] = total[:, 0] + total[:, 1]


def is_odd(axis):
    return (lax.axis_index(axis) & 1) == 1


class Faces:
    def __init__(self, count, layers, breadth, x_low, x_high, y_out, z_first, z_second):
        self.count, self.layers, self.breadth = count, layers, breadth
        self.halves = breadth // ROWS
        self.width = 2 * layers * self.halves
        self.per = LANES // self.width
        self.groups = -(-count // self.per)
        self.x_low, self.x_high, self.y_out = x_low, x_high, y_out
        self.z_first, self.z_second = z_first, z_second

    def start(self):
        return tuple(jnp.zeros((ROWS, LANES), jnp.float32) for _ in range(self.groups))

    def lane(self, f, z, half):
        return (f % self.per) * self.width + 2 * (z * self.halves + half)

    def add(self, carry, f, z, cells, lanes):
        carry = list(carry)
        self.x_low[f, pl.ds(z, 1), :] = cells[:1]
        self.x_high[f, pl.ds(z, 1), :] = cells[-1:]
        group = f // self.per
        for half in range(self.halves):
            k = self.lane(f, z, half)
            turned = pltpu.roll(cells[half * ROWS : (half + 1) * ROWS], k + 1, 1)
            carry[group] = jnp.where((lanes >> 1) == (k >> 1), turned, carry[group])
        return tuple(carry)

    def finish(self, carry, fields, extra):
        for group in range(self.groups):
            self.y_out[group] = carry[group]
        odd = is_odd("gz")
        for f in range(self.count):
            source = fields.at[f] if f < self.count - 1 else extra
            low, high = source[0], source[self.layers - 1]
            self.z_first[f] = jnp.where(odd, low, high)
            self.z_second[f] = jnp.where(odd, high, low)


def split_x(refs, together):
    if together:
        return (refs[0].at[0], refs[0].at[1]), refs[1:]
    return (refs[0], refs[1]), refs[2:]


def pack_kernel(together, grains, solute, mixed, *rest):
    (x_low, x_high), (y_out, z_first, z_second) = split_x(rest, together)
    orders, layers, breadth, _ = grains.shape
    faces = Faces(orders + 1, layers, breadth, x_low, x_high, y_out, z_first, z_second)
    lanes = lax.broadcasted_iota(jnp.int32, (ROWS, LANES), 1)

    def layer(z, carry):
        squares = None
        for f in range(orders):
            cells = grains[f, z]
            squares = cells * cells if squares is None else squares + cells * cells
            carry = faces.add(carry, f, z, cells, lanes)
        value = solute[z] - 0.5 * squares
        mixed[z] = value
        return faces.add(carry, orders, z, value, lanes)

    faces.finish(lax.fori_loop(0, layers, layer, faces.start()), grains, mixed)


def step_kernel(opening, last, together, ring, columns, *refs):
    refs = list(refs)
    take = lambda n: [refs.pop(0) for _ in range(n)]
    fields, solute, mixed = take(3)
    if opening:
        parts = take(ring)
        (parity,) = take(1)
    else:
        (heat,) = take(1)
    if together:
        (arrived,) = take(1)
        x_low, x_high = arrived.at[1], arrived.at[0]
    else:
        x_low, x_high = take(2)
    y_first, y_second, z_first, z_second = take(4)
    fields_out, solute_out = take(2)
    if opening:
        (heat,) = take(1)
    orders, layers, breadth, _ = fields.shape
    count = orders + 1
    if last:
        wide, turned = take(2)
        faces = Faces(count, layers, breadth, None, None, None, None, None)
    else:
        (mixed_out,) = take(1)
        (out_low, out_high), refs = split_x(refs, together)
        out_y, out_z_first, out_z_second, wide, turned = refs
        faces = Faces(count, layers, breadth, out_low, out_high, out_y, out_z_first, out_z_second)
    lanes = lax.broadcasted_iota(jnp.int32, (ROWS, LANES), 1)

    odd_z, odd_y = is_odd("gz"), is_odd("gy")
    for f in range(count):
        source = fields.at[f] if f < orders else mixed
        wide[f, 1 : layers + 1, ROWS : ROWS + breadth, :] = source[...]
        wide[f, 0, ROWS : ROWS + breadth, :] = jnp.where(odd_z, z_first[f], z_second[f])
        wide[f, layers + 1, ROWS : ROWS + breadth, :] = jnp.where(odd_z, z_second[f], z_first[f])
        wide[f, 1 : layers + 1, ROWS - 1, :] = x_low[f]
        wide[f, 1 : layers + 1, ROWS + breadth, :] = x_high[f]
    for group in range(faces.groups):
        first, second = y_first[group], y_second[group]
        below, above = jnp.where(odd_y, first, second), jnp.where(odd_y, second, first)
        turned[group] = jnp.where((lanes & 1) == 1, pltpu.roll(below, 1, 1), pltpu.roll(above, LANES - 1, 1))

    if opening:
        lattice = parts[0][...]
        for part in parts[1:]:
            lattice = lattice + part[...]
        coarse = lattice.astype(jnp.bfloat16).astype(jnp.float32)
        pair = jnp.concatenate([coarse, lattice - coarse], axis=1)
        pair = pair.reshape(columns * 2 * ROWS, LANES).astype(jnp.bfloat16)
        shape = (layers * breadth, columns * 2 * ROWS)
        cell = lax.broadcasted_iota(jnp.int32, shape, 0)
        node = lax.broadcasted_iota(jnp.int32, shape, 1)

        def hat(position, index, odd):
            gap = (position + odd - 2 * index).astype(jnp.float32)
            return jnp.maximum(0.0, 1.0 - 0.5 * jnp.abs(gap))

        weight = hat(cell // breadth, node % ROWS, parity[0]) * hat(cell % breadth, node // (2 * ROWS), parity[1])
        warm = jnp.dot(weight.astype(jnp.bfloat16), pair, preferred_element_type=jnp.float32)
        heat[...] = warm.reshape(layers, breadth, LANES)

    def around(f, z, cells):
        span = slice(ROWS, ROWS + breadth)
        total = wide[f, z, span, :] + wide[f, z + 2, span, :]
        total = total + wide[f, z + 1, ROWS - 1 : ROWS - 1 + breadth, :]
        total = total + wide[f, z + 1, ROWS + 1 : ROWS + 1 + breadth, :]
        sides = []
        for half in range(faces.halves):
            piece = cells[half * ROWS : (half + 1) * ROWS]
            k = faces.lane(f, z, half)
            beyond = pltpu.roll(turned[f // faces.per], LANES - 1 - k, 1)
            below = jnp.where(lanes == 0, beyond, pltpu.roll(piece, 1, 1))
            above = jnp.where(lanes == LANES - 1, beyond, pltpu.roll(piece, LANES - 1, 1))
            sides.append(below + above)
        return total + jnp.concatenate(sides, axis=0)

    def layer(z, carry):
        squares = None
        for f in range(orders):
            cells = fields[f, z]
            squares = cells * cells if squares is None else squares + cells * cells
        here = solute[z]
        pull = 0.04 - 0.1 * squares
        drive = 6.0 * (1.0 - heat[z] - 0.5 * here)
        level = mixed[z]
        fresh = here + 0.15 * (around(orders, z, level) - 6.0 * level)
        solute_out[z] = fresh
        squares = None
        for f in range(orders):
            cells = fields[f, z]
            well = cells * (1.0 - cells)
            value = (
                0.16 * around(f, z, cells)
                + cells * (pull + 0.1 * (cells * cells))
                + well * (drive * well + (0.4 * cells - 0.2))
            )
            fields_out[f, z] = value
            if not last:
                squares = value * value if squares is None else squares + value * value
                carry = faces.add(carry, f, z, value, lanes)
        if last:
            return carry
        value = fresh - 0.5 * squares
        mixed_out[z] = value
        return faces.add(carry, orders, z, value, lanes)

    carry = lax.fori_loop(0, layers, layer, () if last else faces.start())
    if not last:
        faces.finish(carry, fields_out, mixed_out)


def shape_of(*dims, dtype=jnp.float32):
    return jax.ShapeDtypeStruct(dims, dtype)


def cost(flops, moved):
    return pl.CostEstimate(flops=flops, bytes_accessed=moved, transcendentals=0)


def around_ring(axis, distance):
    count = lax.axis_size(axis)
    return [(i, (i + distance) % count) for i in range(count)]


def swaps(axis, closed):
    count = lax.axis_size(axis)
    assert count % 2 == 0
    first = [(i, i ^ 1) for i in range(count)]
    second = [(i, (i + 1 if i % 2 else i - 1) % count) for i in range(count)]
    if not closed:
        second = [(0, 0)] + second[1:-1] + [(count - 1, count - 1)]
    return first, second


def body(grains, solute, thermal, block_slot, block_owner, block_offset):
    ring = lax.axis_size("gz")
    across = lax.axis_size("gx")
    together = across == 2
    orders, layers, breadth, length = grains.shape
    slots = thermal.shape[3]
    capacity = slots // ring
    columns = breadth // 2 + 1
    count = orders + 1
    assert length == LANES and breadth % ROWS == 0 and layers // 2 + 1 <= ROWS

    routed = pl.pallas_call(
        functools.partial(route_kernel, ring, capacity),
        out_shape=[shape_of(4 * capacity, dtype=jnp.int32)] * ring + [shape_of(2, dtype=jnp.int32)],
        in_specs=[SMEM] * 3,
        out_specs=[SMEM] * (ring + 1),
        scratch_shapes=[pltpu.SMEM((block_slot.shape[-1] + 1,), jnp.int32)],
        compiler_params=PARAMS,
        name="route",
    )(block_slot, block_owner, block_offset.reshape(3, 1, -1))
    asked, parity = routed[:ring], routed[ring]
    asked = [asked[0]] + [lax.ppermute(asked[d], "gz", around_ring("gz", d)) for d in range(1, ring)]

    sizes = Faces(count, layers, breadth, None, None, None, None, None)
    face_x = [shape_of(2, count, layers, length)] if together else [shape_of(count, layers, length)] * 2
    face_shapes = face_x + [shape_of(sizes.groups, ROWS, LANES)] + [shape_of(count, breadth, length)] * 2
    tile = shape_of(layers, breadth, length)

    packed = pl.pallas_call(
        functools.partial(pack_kernel, together),
        out_shape=[tile] + face_shapes,
        in_specs=[VMEM] * 2,
        out_specs=[VMEM] * (1 + len(face_shapes)),
        cost_estimate=cost(4_000_000, 2_000_000),
        compiler_params=PARAMS,
        name="pack",
    )(grains, solute)

    def exchange(faces):
        if together:
            moved = [lax.ppermute(faces[0], "gx", around_ring("gx", 1))]
        else:
            moved = [
                lax.ppermute(faces[1], "gx", around_ring("gx", 1)),
                lax.ppermute(faces[0], "gx", around_ring("gx", -1)),
            ]
        y_out, z_first, z_second = faces[-3:]
        return moved + [
            lax.ppermute(y_out, "gy", swaps("gy", True)[0]),
            lax.ppermute(y_out, "gy", swaps("gy", True)[1]),
            lax.ppermute(z_first, "gz", swaps("gz", False)[0]),
            lax.ppermute(z_second, "gz", swaps("gz", False)[1]),
        ]

    mixed, faces = packed[0], packed[1:]
    arrived = exchange(faces)

    nodes = thermal.reshape(slots, NODES, NODES * NODES)
    lattice = shape_of(columns, ROWS, length)
    parts = pl.pallas_call(
        functools.partial(project_kernel, ring, capacity, columns),
        out_shape=[lattice] * ring,
        in_specs=[SMEM] * ring + [VMEM],
        out_specs=[VMEM] * ring,
        cost_estimate=cost(4_000_000, 1_000_000),
        compiler_params=PARAMS,
        name="project",
    )(*asked, nodes)
    parts = [parts[0]] + [lax.ppermute(parts[d], "gz", around_ring("gz", -d)) for d in range(1, ring)]

    fields = grains
    heat = None
    for repeat in range(STEPS):
        first, last = repeat == 0, repeat == STEPS - 1
        extra = list(parts) + [parity] if first else [heat]
        extra_specs = [VMEM] * ring + [SMEM] if first else [VMEM]
        out_shape = [shape_of(*grains.shape), tile]
        if first:
            out_shape = out_shape + [tile]
        if not last:
            out_shape = out_shape + [tile] + face_shapes
        outs = pl.pallas_call(
            functools.partial(step_kernel, first, last, together, ring, columns),
            out_shape=out_shape,
            in_specs=[VMEM] * 3 + extra_specs + [VMEM] * len(arrived),
            out_specs=[VMEM] * len(out_shape),
            scratch_shapes=[
                pltpu.VMEM((count, layers + 2, breadth + 2 * ROWS, LANES), jnp.float32),
                pltpu.VMEM((sizes.groups, ROWS, LANES), jnp.float32),
            ],
            cost_estimate=cost(8_000_000, 3_000_000),
            compiler_params=PARAMS,
            name=f"step{repeat}",
        )(fields, solute, mixed, *extra, *arrived)
        fields, solute = outs[:2]
        outs = list(outs[2:])
        if first:
            heat = outs.pop(0)
        if not last:
            mixed, faces = outs[0], outs[1:]
            arrived = exchange(faces)
    return (fields, solute, heat)


def solution(mesh):
    in_specs = (
        P(None, "gz", "gx", "gy"),
        P("gz", "gx", "gy"),
        P("gz", "gx", "gy", None, None),
        P("gz", "gx", "gy", None),
        P("gz", "gx", "gy", None),
        P("gz", "gx", "gy", None, None),
    )
    out_specs = (P(None, "gz", "gx", "gy"), P("gz", "gx", "gy"), P("gz", "gx", "gy"))
    return jax.shard_map(body, mesh=mesh, in_specs=in_specs, out_specs=out_specs, check_vma=False)
```

```python
import functools

import jax
import jax.numpy as jnp
from jax import lax
from jax.experimental import pallas as pl
from jax.experimental.pallas import tpu as pltpu
from jax.sharding import PartitionSpec as P


NODES = 16
STEPS = 3
LANES = 128
ROWS = 8
FAR = 4096

VMEM = pl.BlockSpec(memory_space=pltpu.VMEM)
HBM = pl.BlockSpec(memory_space=pltpu.HBM)
SMEM = pl.BlockSpec(memory_space=pltpu.SMEM)

PARAMS = pltpu.CompilerParams(vmem_limit_bytes=12 * 1024 * 1024)


def log2(size):
    assert size & (size - 1) == 0
    return size.bit_length() - 1


def half_up(start):
    return (start + (start & 1)) >> 1


def route_kernel(ring, capacity, *refs):
    lists, parity, picks = refs[3 : 3 + ring], refs[3 + ring], refs[4 + ring]
    slot_ref, owner_ref, start_ref, arrivals = refs[5 + ring :]
    copies = [
        pltpu.make_async_copy(source, target, arrivals.at[i])
        for i, (source, target) in enumerate(zip(refs[:3], (slot_ref, owner_ref, start_ref)))
    ]
    for copy in copies:
        copy.start()
    for copy in copies:
        copy.wait()
    entries = slot_ref.shape[-1]
    me = lax.axis_index("gz")
    owners = [owner_ref[0, 0, 0, e] for e in range(entries)]
    for axis in range(2):
        odd = jnp.int32(0)
        for e in range(entries):
            odd = odd | jnp.where(owners[e] >= 0, start_ref[axis, 0, e] & 1, 0)
        parity[axis] = odd
    for distance in range(ring):
        target = lax.rem(me + distance, ring)
        found = jnp.int32(0)
        for e in range(entries):
            picks[found] = e
            found = found + (owners[e] == target).astype(jnp.int32)
        for c in range(capacity):
            held = c < found
            e = jnp.where(held, picks[c], 0)
            lists[distance][4 * c] = jnp.maximum(slot_ref[0, 0, 0, e], 0)
            for axis in range(3):
                lists[distance][4 * c + 1 + axis] = jnp.where(held, start_ref[axis, 0, e], FAR)


def project_kernel(ring, capacity, columns, *refs):
    lists, thermal, outs, both = refs[:ring], refs[ring], refs[ring + 1 : -1], refs[-1]
    tall = 2 * ROWS
    shape = (2 * tall, LANES)
    row = lax.broadcasted_iota(jnp.int32, shape, 0)
    node_x = ((row & 1) << 3) + (lax.broadcasted_iota(jnp.int32, shape, 1) >> log2(NODES))
    plane = lax.broadcasted_iota(jnp.int32, (tall, LANES), 0) >> 1
    cell_y = lax.broadcasted_iota(jnp.int32, (NODES, LANES), 1)
    node_y = 2 * lax.broadcasted_iota(jnp.int32, (NODES, LANES), 0)
    for distance in range(ring):
        total = None
        for c in range(capacity):
            slot, z, x, y = (lists[distance][4 * c + i] for i in range(4))
            rise = half_up(z)
            planes = pltpu.roll(thermal[slot], (2 * rise) & (2 * NODES - 1), 0)[:tall]
            planes = jnp.where((plane >= rise) & (plane < rise + NODES), planes, 0.0)
            coarse = planes.astype(jnp.bfloat16).astype(jnp.float32)
            pair = jnp.concatenate([coarse, planes - coarse], axis=0).astype(jnp.bfloat16)
            shift = half_up(x)
            spread = jnp.concatenate(
                [pair * (node_x == j - shift).astype(jnp.float32).astype(jnp.bfloat16) for j in range(columns)],
                axis=0,
            )
            distance_y = (cell_y - y - node_y).astype(jnp.float32)
            hat = jnp.maximum(0.0, 1.0 - 0.5 * jnp.abs(distance_y)).astype(jnp.bfloat16)
            weight = jnp.concatenate([hat] * (LANES // NODES), axis=0)
            part = jnp.dot(spread, weight, preferred_element_type=jnp.float32)
            total = part if total is None else total + part
        total = total.reshape(columns, 2, tall, LANES)
        both[distance] = (total[:, 0] + total[:, 1]).reshape(columns * tall, LANES)
        even, odd = (both[distance, pl.ds(i, columns * ROWS, stride=2), :] for i in range(2))
        outs[distance][...] = (even + odd).reshape(columns, ROWS, LANES)


def is_odd(axis):
    return (lax.axis_index(axis) & 1) == 1


class Faces:
    def __init__(self, count, layers, breadth, x_low, x_high, y_out, z_first, z_second):
        self.count, self.layers, self.breadth = count, layers, breadth
        self.halves = breadth // ROWS
        self.width = 2 * layers * self.halves
        self.per = LANES // self.width
        self.groups = -(-count // self.per)
        self.x_low, self.x_high, self.y_out = x_low, x_high, y_out
        self.z_first, self.z_second = z_first, z_second

    def lane(self, f, z, half):
        return (f % self.per) * self.width + 2 * (z * self.halves + half)

    def pack(self, fields, extra):
        lanes = lax.broadcasted_iota(jnp.int32, (ROWS, LANES), 1)
        odd = is_odd("gz")
        packed = [None] * self.groups
        for f in range(self.count):
            source = fields.at[f] if f < self.count - 1 else extra
            flat = source.reshape(self.layers * self.breadth, LANES)
            self.x_low[f] = flat[pl.ds(0, self.layers, stride=self.breadth), :]
            self.x_high[f] = flat[pl.ds(self.breadth - 1, self.layers, stride=self.breadth), :]
            low, high = source[0], source[self.layers - 1]
            self.z_first[f] = jnp.where(odd, low, high)
            self.z_second[f] = jnp.where(odd, high, low)
            group = f // self.per
            for z in range(self.layers):
                for half in range(self.halves):
                    k = self.lane(f, z, half)
                    turned = pltpu.roll(source[z, half * ROWS : (half + 1) * ROWS, :], k + 1, 1)
                    known = packed[group]
                    packed[group] = turned if known is None else jnp.where(lanes >> 1 == k >> 1, turned, known)
        for group in range(self.groups):
            self.y_out[group] = packed[group]


def split_x(refs, together):
    if together:
        return (refs[0].at[0], refs[0].at[1]), refs[1:]
    return (refs[0], refs[1]), refs[2:]


def pack_kernel(together, grains, solute, mixed, *rest):
    (x_low, x_high), (y_out, z_first, z_second) = split_x(rest, together)
    orders, layers, breadth, _ = grains.shape
    for z in range(layers):
        squares = None
        for f in range(orders):
            cells = grains[f, z]
            squares = cells * cells if squares is None else squares + cells * cells
        mixed[z] = solute[z] - 0.5 * squares
    Faces(orders + 1, layers, breadth, x_low, x_high, y_out, z_first, z_second).pack(grains, mixed)


def step_kernel(opening, last, together, ring, columns, *refs):
    refs = list(refs)
    take = lambda n: [refs.pop(0) for _ in range(n)]
    fields, solute, mixed = take(3)
    if opening:
        parts = take(ring)
        (parity,) = take(1)
    else:
        (heat,) = take(1)
    if together:
        (arrived,) = take(1)
        x_low, x_high = arrived.at[1], arrived.at[0]
    else:
        x_low, x_high = take(2)
    y_first, y_second, z_first, z_second = take(4)
    fields_out, solute_out = take(2)
    if opening:
        (heat,) = take(1)
    if last:
        (heat_out,) = take(1)
        heat_out[...] = heat[...]
    orders, layers, breadth, _ = fields.shape
    count = orders + 1
    if last:
        wide, turned = take(2)
        faces = Faces(count, layers, breadth, None, None, None, None, None)
    else:
        (mixed_out,) = take(1)
        (out_low, out_high), refs = split_x(refs, together)
        out_y, out_z_first, out_z_second, wide, turned = refs
        faces = Faces(count, layers, breadth, out_low, out_high, out_y, out_z_first, out_z_second)
    lanes = lax.broadcasted_iota(jnp.int32, (ROWS, LANES), 1)

    odd_z, odd_y = is_odd("gz"), is_odd("gy")
    for f in range(count):
        source = fields.at[f] if f < orders else mixed
        wide[f, 1 : layers + 1, ROWS : ROWS + breadth, :] = source[...]
        wide[f, 0, ROWS : ROWS + breadth, :] = jnp.where(odd_z, z_first[f], z_second[f])
        wide[f, layers + 1, ROWS : ROWS + breadth, :] = jnp.where(odd_z, z_second[f], z_first[f])
        wide[f, 1 : layers + 1, ROWS - 1, :] = x_low[f]
        wide[f, 1 : layers + 1, ROWS + breadth, :] = x_high[f]
    for group in range(faces.groups):
        first, second = y_first[group], y_second[group]
        below, above = jnp.where(odd_y, first, second), jnp.where(odd_y, second, first)
        turned[group] = jnp.where((lanes & 1) == 1, pltpu.roll(below, 1, 1), pltpu.roll(above, LANES - 1, 1))

    if opening:
        lattice = parts[0][...]
        for part in parts[1:]:
            lattice = lattice + part[...]
        coarse = lattice.astype(jnp.bfloat16).astype(jnp.float32)
        pair = jnp.concatenate([coarse, lattice - coarse], axis=1)
        pair = pair.reshape(columns * 2 * ROWS, LANES).astype(jnp.bfloat16)
        shape = (layers * breadth, columns * 2 * ROWS)
        cell = lax.broadcasted_iota(jnp.int32, shape, 0)
        node = lax.broadcasted_iota(jnp.int32, shape, 1)

        def hat(position, index, odd):
            gap = (position + odd - 2 * index).astype(jnp.float32)
            return jnp.maximum(0.0, 1.0 - 0.5 * jnp.abs(gap))

        weight = hat(cell >> log2(breadth), node & (ROWS - 1), parity[0]) * hat(
            cell & (breadth - 1), node >> log2(2 * ROWS), parity[1]
        )
        warm = jnp.dot(weight.astype(jnp.bfloat16), pair, preferred_element_type=jnp.float32)
        heat[...] = warm.reshape(layers, breadth, LANES)

    def around(f, z, cells):
        span = slice(ROWS, ROWS + breadth)
        total = wide[f, z, span, :] + wide[f, z + 2, span, :]
        total = total + wide[f, z + 1, ROWS - 1 : ROWS - 1 + breadth, :]
        total = total + wide[f, z + 1, ROWS + 1 : ROWS + 1 + breadth, :]
        sides = []
        for half in range(faces.halves):
            piece = cells[half * ROWS : (half + 1) * ROWS]
            k = faces.lane(f, z, half)
            beyond = pltpu.roll(turned[f // faces.per], LANES - 1 - k, 1)
            below = jnp.where(lanes == 0, beyond, pltpu.roll(piece, 1, 1))
            above = jnp.where(lanes == LANES - 1, beyond, pltpu.roll(piece, LANES - 1, 1))
            sides.append(below + above)
        return total + jnp.concatenate(sides, axis=0)

    def layer(z):
        squares = None
        for f in range(orders):
            cells = fields[f, z]
            squares = cells * cells if squares is None else squares + cells * cells
        here = solute[z]
        pull = 0.04 - 0.1 * squares
        drive = 6.0 * (1.0 - heat[z] - 0.5 * here)
        level = mixed[z]
        fresh = here + 0.15 * (around(orders, z, level) - 6.0 * level)
        solute_out[z] = fresh
        squares = None
        for f in range(orders):
            cells = fields[f, z]
            well = cells * (1.0 - cells)
            value = (
                0.16 * around(f, z, cells)
                + cells * (pull + 0.1 * (cells * cells))
                + well * (drive * well + (0.4 * cells - 0.2))
            )
            fields_out[f, z] = value
            if not last:
                squares = value * value if squares is None else squares + value * value
        if not last:
            mixed_out[z] = fresh - 0.5 * squares

    for z in range(layers):
        layer(z)
    if not last:
        faces.pack(fields_out, mixed_out)


def shape_of(*dims, dtype=jnp.float32):
    return jax.ShapeDtypeStruct(dims, dtype)


def cost(flops, moved):
    return pl.CostEstimate(flops=flops, bytes_accessed=moved, transcendentals=0)


def around_ring(axis, distance):
    count = lax.axis_size(axis)
    return [(i, (i + distance) % count) for i in range(count)]


def send(value, axis, pairs):
    return lax.ppermute(value, axis, pairs)


def swaps(axis, closed):
    count = lax.axis_size(axis)
    assert count % 2 == 0
    first = [(i, i ^ 1) for i in range(count)]
    second = [(i, (i + 1 if i % 2 else i - 1) % count) for i in range(count)]
    if not closed:
        second = [(0, 0)] + second[1:-1] + [(count - 1, count - 1)]
    return first, second


def body(grains, solute, thermal, block_slot, block_owner, block_offset):
    ring = lax.axis_size("gz")
    across = lax.axis_size("gx")
    together = across == 2
    orders, layers, breadth, length = grains.shape
    slots = thermal.shape[3]
    capacity = slots // ring
    columns = breadth // 2 + 1
    count = orders + 1
    entries = block_slot.shape[-1]
    assert length == LANES and breadth % ROWS == 0 and layers // 2 + 1 <= ROWS

    routed = pl.pallas_call(
        functools.partial(route_kernel, ring, capacity),
        out_shape=[shape_of(4 * capacity, dtype=jnp.int32)] * ring + [shape_of(2, dtype=jnp.int32)],
        in_specs=[HBM] * 3,
        out_specs=[SMEM] * (ring + 1),
        scratch_shapes=[
            pltpu.SMEM((entries + 1,), jnp.int32),
            pltpu.SMEM(block_slot.shape, jnp.int32),
            pltpu.SMEM(block_owner.shape, jnp.int32),
            pltpu.SMEM((3, 1, entries), jnp.int32),
            pltpu.SemaphoreType.DMA((3,)),
        ],
        name="route",
    )(block_slot, block_owner, block_offset.reshape(3, 1, entries))
    asked, parity = routed[:ring], routed[ring]
    asked = [asked[0]] + [send(asked[d], "gz", around_ring("gz", d)) for d in range(1, ring)]

    sizes = Faces(count, layers, breadth, None, None, None, None, None)
    face_x = [shape_of(2, count, layers, length)] if together else [shape_of(count, layers, length)] * 2
    face_shapes = face_x + [shape_of(sizes.groups, ROWS, LANES)] + [shape_of(count, breadth, length)] * 2
    tile = shape_of(layers, breadth, length)

    packed = pl.pallas_call(
        functools.partial(pack_kernel, together),
        out_shape=[tile] + face_shapes,
        in_specs=[VMEM] * 2,
        out_specs=[VMEM] * (1 + len(face_shapes)),
        cost_estimate=cost(4_000_000, 2_000_000),
        compiler_params=PARAMS,
        name="pack",
    )(grains, solute)

    def exchange(faces):
        y_out, z_first, z_second = faces[-3:]
        y_swaps, z_swaps = swaps("gy", True), swaps("gz", False)
        if together:
            moved = [send(faces[0], "gx", around_ring("gx", 1))]
        else:
            moved = [send(faces[1], "gx", around_ring("gx", 1)), send(faces[0], "gx", around_ring("gx", -1))]
        return moved + [
            send(y_out, "gy", y_swaps[0]),
            send(y_out, "gy", y_swaps[1]),
            send(z_first, "gz", z_swaps[0]),
            send(z_second, "gz", z_swaps[1]),
        ]

    mixed, faces = packed[0], packed[1:]
    arrived = exchange(faces)

    nodes = thermal.reshape(slots, NODES**3 // LANES, LANES)
    assert NODES**2 == 2 * LANES
    lattice = shape_of(columns, ROWS, length)
    parts = pl.pallas_call(
        functools.partial(project_kernel, ring, capacity, columns),
        out_shape=[lattice] * ring,
        in_specs=[SMEM] * ring + [VMEM],
        out_specs=[VMEM] * ring,
        scratch_shapes=[pltpu.VMEM((ring, columns * 2 * ROWS, LANES), jnp.float32)],
        cost_estimate=cost(4_000_000, 1_000_000),
        compiler_params=PARAMS,
        name="project",
    )(*asked, nodes)
    parts = [parts[0]] + [send(parts[d], "gz", around_ring("gz", -d)) for d in range(1, ring)]

    fields, heat = grains, None
    for repeat in range(STEPS):
        first, last = repeat == 0, repeat == STEPS - 1
        extra = list(parts) + [parity] if first else [heat]
        extra_specs = [VMEM] * ring + [SMEM] if first else [VMEM]
        out_shape = [shape_of(*grains.shape), tile]
        if first or last:
            out_shape = out_shape + [tile]
        if not last:
            out_shape = out_shape + [tile] + face_shapes
        outs = pl.pallas_call(
            functools.partial(step_kernel, first, last, together, ring, columns),
            out_shape=out_shape,
            in_specs=[VMEM] * 3 + extra_specs + [VMEM] * len(arrived),
            out_specs=[VMEM] * len(out_shape),
            scratch_shapes=[
                pltpu.VMEM((count, layers + 2, breadth + 2 * ROWS, LANES), jnp.float32),
                pltpu.VMEM((sizes.groups, ROWS, LANES), jnp.float32),
            ],
            cost_estimate=cost(8_000_000, 3_000_000),
            compiler_params=PARAMS,
        )(fields, solute, mixed, *extra, *arrived)
        fields, solute = outs[:2]
        outs = list(outs[2:])
        if first or last:
            heat = outs.pop(0)
        if not last:
            mixed, faces = outs[0], outs[1:]
            arrived = exchange(faces)
    return (fields, solute, heat)


def solution(mesh):
    in_specs = (
        P(None, "gz", "gx", "gy"),
        P("gz", "gx", "gy"),
        P("gz", "gx", "gy", None, None),
        P("gz", "gx", "gy", None),
        P("gz", "gx", "gy", None),
        P("gz", "gx", "gy", None, None),
    )
    out_specs = (P(None, "gz", "gx", "gy"), P("gz", "gx", "gy"), P("gz", "gx", "gy"))

    return jax.shard_map(body, mesh=mesh, in_specs=in_specs, out_specs=out_specs, check_vma=False)
```

```python
import functools

import jax
import jax.numpy as jnp
from jax import lax
from jax.experimental import pallas as pl
from jax.experimental.pallas import tpu as pltpu
from jax.sharding import PartitionSpec as P


NODES = 16
STEPS = 3
LANES = 128
ROWS = 8
FAR = 4096

VMEM = pl.BlockSpec(memory_space=pltpu.VMEM)
HBM = pl.BlockSpec(memory_space=pltpu.HBM)
SMEM = pl.BlockSpec(memory_space=pltpu.SMEM)

PARAMS = pltpu.CompilerParams(vmem_limit_bytes=12 * 1024 * 1024)


def log2(size):
    assert size & (size - 1) == 0
    return size.bit_length() - 1


def half_up(start):
    return (start + (start & 1)) >> 1


def route_kernel(ring, capacity, table, *refs):
    lists, parity, picks = refs[:ring], refs[ring], refs[ring + 1]
    entries = table.shape[-1]
    me = lax.axis_index("gz")
    owners = [table[1, 0, e] for e in range(entries)]
    for axis in range(2):
        odd = jnp.int32(0)
        for e in range(entries):
            odd = odd | jnp.where(owners[e] >= 0, table[2 + axis, 0, e] & 1, 0)
        parity[axis] = odd
    for distance in range(ring):
        target = lax.rem(me + distance, ring)
        found = jnp.int32(0)
        for e in range(entries):
            picks[found] = e
            found = found + (owners[e] == target).astype(jnp.int32)
        for c in range(capacity):
            held = c < found
            e = jnp.where(held, picks[c], 0)
            lists[distance][4 * c] = jnp.maximum(table[0, 0, e], 0)
            for axis in range(3):
                lists[distance][4 * c + 1 + axis] = jnp.where(held, table[2 + axis, 0, e], FAR)


def project_kernel(ring, capacity, columns, *refs):
    lists, thermal, outs, both = refs[:ring], refs[ring], refs[ring + 1 : -1], refs[-1]
    tall = 2 * ROWS
    shape = (2 * tall, LANES)
    row = lax.broadcasted_iota(jnp.int32, shape, 0)
    node_x = ((row & 1) << 3) + (lax.broadcasted_iota(jnp.int32, shape, 1) >> log2(NODES))
    plane = lax.broadcasted_iota(jnp.int32, (tall, LANES), 0) >> 1
    cell_y = lax.broadcasted_iota(jnp.int32, (NODES, LANES), 1)
    node_y = 2 * lax.broadcasted_iota(jnp.int32, (NODES, LANES), 0)
    for distance in range(ring):
        total = None
        for c in range(capacity):
            slot, z, x, y = (lists[distance][4 * c + i] for i in range(4))
            rise = half_up(z)
            planes = pltpu.roll(thermal[slot], (2 * rise) & (2 * NODES - 1), 0)[:tall]
            planes = jnp.where((plane >= rise) & (plane < rise + NODES), planes, 0.0)
            coarse = planes.astype(jnp.bfloat16).astype(jnp.float32)
            pair = jnp.concatenate([coarse, planes - coarse], axis=0).astype(jnp.bfloat16)
            shift = half_up(x)
            spread = jnp.concatenate(
                [pair * (node_x == j - shift).astype(jnp.float32).astype(jnp.bfloat16) for j in range(columns)],
                axis=0,
            )
            distance_y = (cell_y - y - node_y).astype(jnp.float32)
            hat = jnp.maximum(0.0, 1.0 - 0.5 * jnp.abs(distance_y)).astype(jnp.bfloat16)
            weight = jnp.concatenate([hat] * (LANES // NODES), axis=0)
            part = jnp.dot(spread, weight, preferred_element_type=jnp.float32)
            total = part if total is None else total + part
        total = total.reshape(columns, 2, tall, LANES)
        both[distance] = (total[:, 0] + total[:, 1]).reshape(columns * tall, LANES)
        even, odd = (both[distance, pl.ds(i, columns * ROWS, stride=2), :] for i in range(2))
        outs[distance][...] = (even + odd).reshape(columns, ROWS, LANES)


def is_odd(axis):
    return (lax.axis_index(axis) & 1) == 1


class Faces:
    def __init__(self, count, layers, breadth, x_low, x_high, y_out, z_first, z_second):
        self.count, self.layers, self.breadth = count, layers, breadth
        self.halves = breadth // ROWS
        self.width = 2 * layers * self.halves
        self.per = LANES // self.width
        self.groups = -(-count // self.per)
        self.x_low, self.x_high, self.y_out = x_low, x_high, y_out
        self.z_first, self.z_second = z_first, z_second

    def lane(self, f, z, half):
        return (f % self.per) * self.width + 2 * (z * self.halves + half)

    def pack(self, fields, extra):
        lanes = lax.broadcasted_iota(jnp.int32, (ROWS, LANES), 1)
        odd = is_odd("gz")
        packed = [None] * self.groups
        for f in range(self.count):
            source = fields.at[f] if f < self.count - 1 else extra
            flat = source.reshape(self.layers * self.breadth, LANES)
            self.x_low[f] = flat[pl.ds(0, self.layers, stride=self.breadth), :]
            self.x_high[f] = flat[pl.ds(self.breadth - 1, self.layers, stride=self.breadth), :]
            low, high = source[0], source[self.layers - 1]
            self.z_first[f] = jnp.where(odd, low, high)
            self.z_second[f] = jnp.where(odd, high, low)
            group = f // self.per
            for z in range(self.layers):
                for half in range(self.halves):
                    k = self.lane(f, z, half)
                    turned = pltpu.roll(source[z, half * ROWS : (half + 1) * ROWS, :], k + 1, 1)
                    known = packed[group]
                    packed[group] = turned if known is None else jnp.where(lanes >> 1 == k >> 1, turned, known)
        for group in range(self.groups):
            self.y_out[group] = packed[group]


def split_x(refs, together):
    if together:
        return (refs[0].at[0], refs[0].at[1]), refs[1:]
    return (refs[0], refs[1]), refs[2:]


def pack_kernel(together, grains, solute, mixed, *rest):
    (x_low, x_high), (y_out, z_first, z_second) = split_x(rest, together)
    orders, layers, breadth, _ = grains.shape
    for z in range(layers):
        squares = None
        for f in range(orders):
            cells = grains[f, z]
            squares = cells * cells if squares is None else squares + cells * cells
        mixed[z] = solute[z] - 0.5 * squares
    Faces(orders + 1, layers, breadth, x_low, x_high, y_out, z_first, z_second).pack(grains, mixed)


def step_kernel(opening, last, together, ring, columns, *refs):
    refs = list(refs)
    take = lambda n: [refs.pop(0) for _ in range(n)]
    fields, solute, mixed = take(3)
    if opening:
        parts = take(ring)
        (parity,) = take(1)
    else:
        (heat,) = take(1)
    if together:
        (arrived,) = take(1)
        x_low, x_high = arrived.at[1], arrived.at[0]
    else:
        x_low, x_high = take(2)
    y_first, y_second, z_first, z_second = take(4)
    fields_out, solute_out = take(2)
    if opening:
        (heat,) = take(1)
    if last:
        (heat_out,) = take(1)
        far = fields_out, solute_out
        leaving, fields_out, solute_out = refs.pop(), refs.pop(), refs.pop()
    orders, layers, breadth, _ = fields.shape
    count = orders + 1
    if last:
        wide, turned = take(2)
        faces = Faces(count, layers, breadth, None, None, None, None, None)
    else:
        (mixed_out,) = take(1)
        (out_low, out_high), refs = split_x(refs, together)
        out_y, out_z_first, out_z_second, wide, turned = refs
        faces = Faces(count, layers, breadth, out_low, out_high, out_y, out_z_first, out_z_second)
    lanes = lax.broadcasted_iota(jnp.int32, (ROWS, LANES), 1)

    odd_z, odd_y = is_odd("gz"), is_odd("gy")
    for f in range(count):
        source = fields.at[f] if f < orders else mixed
        wide[f, 1 : layers + 1, ROWS : ROWS + breadth, :] = source[...]
        wide[f, 0, ROWS : ROWS + breadth, :] = jnp.where(odd_z, z_first[f], z_second[f])
        wide[f, layers + 1, ROWS : ROWS + breadth, :] = jnp.where(odd_z, z_second[f], z_first[f])
        wide[f, 1 : layers + 1, ROWS - 1, :] = x_low[f]
        wide[f, 1 : layers + 1, ROWS + breadth, :] = x_high[f]
    for group in range(faces.groups):
        first, second = y_first[group], y_second[group]
        below, above = jnp.where(odd_y, first, second), jnp.where(odd_y, second, first)
        turned[group] = jnp.where((lanes & 1) == 1, pltpu.roll(below, 1, 1), pltpu.roll(above, LANES - 1, 1))

    if opening:
        lattice = parts[0][...]
        for part in parts[1:]:
            lattice = lattice + part[...]
        coarse = lattice.astype(jnp.bfloat16).astype(jnp.float32)
        pair = jnp.concatenate([coarse, lattice - coarse], axis=1)
        pair = pair.reshape(columns * 2 * ROWS, LANES).astype(jnp.bfloat16)
        shape = (layers * breadth, columns * 2 * ROWS)
        cell = lax.broadcasted_iota(jnp.int32, shape, 0)
        node = lax.broadcasted_iota(jnp.int32, shape, 1)

        def hat(position, index, odd):
            gap = (position + odd - 2 * index).astype(jnp.float32)
            return jnp.maximum(0.0, 1.0 - 0.5 * jnp.abs(gap))

        weight = hat(cell >> log2(breadth), node & (ROWS - 1), parity[0]) * hat(
            cell & (breadth - 1), node >> log2(2 * ROWS), parity[1]
        )
        warm = jnp.dot(weight.astype(jnp.bfloat16), pair, preferred_element_type=jnp.float32)
        heat[...] = warm.reshape(layers, breadth, LANES)

    def around(f, z, cells):
        span = slice(ROWS, ROWS + breadth)
        total = wide[f, z, span, :] + wide[f, z + 2, span, :]
        total = total + wide[f, z + 1, ROWS - 1 : ROWS - 1 + breadth, :]
        total = total + wide[f, z + 1, ROWS + 1 : ROWS + 1 + breadth, :]
        sides = []
        for half in range(faces.halves):
            piece = cells[half * ROWS : (half + 1) * ROWS]
            k = faces.lane(f, z, half)
            beyond = pltpu.roll(turned[f // faces.per], LANES - 1 - k, 1)
            below = jnp.where(lanes == 0, beyond, pltpu.roll(piece, 1, 1))
            above = jnp.where(lanes == LANES - 1, beyond, pltpu.roll(piece, LANES - 1, 1))
            sides.append(below + above)
        return total + jnp.concatenate(sides, axis=0)

    def layer(z):
        squares = None
        for f in range(orders):
            cells = fields[f, z]
            squares = cells * cells if squares is None else squares + cells * cells
        here = solute[z]
        pull = 0.04 - 0.1 * squares
        drive = 6.0 * (1.0 - heat[z] - 0.5 * here)
        level = mixed[z]
        fresh = here + 0.15 * (around(orders, z, level) - 6.0 * level)
        solute_out[z] = fresh
        squares = None
        for f in range(orders):
            cells = fields[f, z]
            well = cells * (1.0 - cells)
            value = (
                0.16 * around(f, z, cells)
                + cells * (pull + 0.1 * (cells * cells))
                + well * (drive * well + (0.4 * cells - 0.2))
            )
            fields_out[f, z] = value
            if not last:
                squares = value * value if squares is None else squares + value * value
        if not last:
            mixed_out[z] = fresh - 0.5 * squares

    copies = []
    if last:
        copies.append(pltpu.make_async_copy(heat, heat_out, leaving.at[layers]))
        copies[-1].start()
    for z in range(layers):
        layer(z)
        if last:
            copies.append(pltpu.make_async_copy(fields_out.at[:, z], far[0].at[:, z], leaving.at[z]))
            copies[-1].start()
    if last:
        copies.append(pltpu.make_async_copy(solute_out, far[1], leaving.at[layers + 1]))
        copies[-1].start()
        for copy in copies:
            copy.wait()
    else:
        faces.pack(fields_out, mixed_out)


def shape_of(*dims, dtype=jnp.float32):
    return jax.ShapeDtypeStruct(dims, dtype)


def cost(flops, moved):
    return pl.CostEstimate(flops=flops, bytes_accessed=moved, transcendentals=0)


def around_ring(axis, distance):
    count = lax.axis_size(axis)
    return [(i, (i + distance) % count) for i in range(count)]


def send(value, axis, pairs):
    return lax.ppermute(value, axis, pairs)


def swaps(axis, closed):
    count = lax.axis_size(axis)
    assert count % 2 == 0
    first = [(i, i ^ 1) for i in range(count)]
    second = [(i, (i + 1 if i % 2 else i - 1) % count) for i in range(count)]
    if not closed:
        second = [(0, 0)] + second[1:-1] + [(count - 1, count - 1)]
    return first, second


def body(grains, solute, thermal, block_slot, block_owner, block_offset):
    ring = lax.axis_size("gz")
    across = lax.axis_size("gx")
    together = across == 2
    orders, layers, breadth, length = grains.shape
    slots = thermal.shape[3]
    capacity = slots // ring
    columns = breadth // 2 + 1
    count = orders + 1
    entries = block_slot.shape[-1]
    assert length == LANES and breadth % ROWS == 0 and layers // 2 + 1 <= ROWS

    table = jnp.concatenate(
        [array.reshape(-1, 1, entries) for array in (block_slot, block_owner, block_offset)], axis=0
    )
    routed = pl.pallas_call(
        functools.partial(route_kernel, ring, capacity),
        out_shape=[shape_of(4 * capacity, dtype=jnp.int32)] * ring + [shape_of(2, dtype=jnp.int32)],
        in_specs=[SMEM],
        out_specs=[SMEM] * (ring + 1),
        scratch_shapes=[pltpu.SMEM((entries + 1,), jnp.int32)],
        compiler_params=PARAMS,
        cost_estimate=cost(1_000_000_000, 1_000),
        name="route",
    )(table)
    asked, parity = routed[:ring], routed[ring]
    asked = [asked[0]] + [send(asked[d], "gz", around_ring("gz", d)) for d in range(1, ring)]

    sizes = Faces(count, layers, breadth, None, None, None, None, None)
    face_x = [shape_of(2, count, layers, length)] if together else [shape_of(count, layers, length)] * 2
    face_shapes = face_x + [shape_of(sizes.groups, ROWS, LANES)] + [shape_of(count, breadth, length)] * 2
    tile = shape_of(layers, breadth, length)

    packed = pl.pallas_call(
        functools.partial(pack_kernel, together),
        out_shape=[tile] + face_shapes,
        in_specs=[VMEM] * 2,
        out_specs=[VMEM] * (1 + len(face_shapes)),
        cost_estimate=cost(400_000_000, 2_000_000),
        compiler_params=PARAMS,
        name="pack",
    )(grains, solute)

    def exchange(faces):
        y_out, z_first, z_second = faces[-3:]
        y_swaps, z_swaps = swaps("gy", True), swaps("gz", False)
        if together:
            moved = [send(faces[0], "gx", around_ring("gx", 1))]
        else:
            moved = [send(faces[1], "gx", around_ring("gx", 1)), send(faces[0], "gx", around_ring("gx", -1))]
        return moved + [
            send(y_out, "gy", y_swaps[0]),
            send(y_out, "gy", y_swaps[1]),
            send(z_first, "gz", z_swaps[0]),
            send(z_second, "gz", z_swaps[1]),
        ]

    mixed, faces = packed[0], packed[1:]
    arrived = exchange(faces)

    nodes = thermal.reshape(slots, NODES**3 // LANES, LANES)
    assert NODES**2 == 2 * LANES
    lattice = shape_of(columns, ROWS, length)
    parts = pl.pallas_call(
        functools.partial(project_kernel, ring, capacity, columns),
        out_shape=[lattice] * ring,
        in_specs=[SMEM] * ring + [VMEM],
        out_specs=[VMEM] * ring,
        scratch_shapes=[pltpu.VMEM((ring, columns * 2 * ROWS, LANES), jnp.float32)],
        cost_estimate=cost(4_000_000, 1_000_000),
        compiler_params=PARAMS,
        name="project",
    )(*asked, nodes)
    parts = [parts[0]] + [send(parts[d], "gz", around_ring("gz", -d)) for d in range(1, ring)]

    fields, heat = grains, None
    leaving = [
        pltpu.VMEM((layers, breadth, length), jnp.float32),
        pltpu.VMEM(grains.shape, jnp.float32),
        pltpu.SemaphoreType.DMA((layers + 2,)),
    ]
    for repeat in range(STEPS):
        first, last = repeat == 0, repeat == STEPS - 1
        extra = list(parts) + [parity] if first else [heat]
        extra_specs = [VMEM] * ring + [SMEM] if first else [VMEM]
        out_shape = [shape_of(*grains.shape), tile]
        if first or last:
            out_shape = out_shape + [tile]
        if not last:
            out_shape = out_shape + [tile] + face_shapes
        outs = pl.pallas_call(
            functools.partial(step_kernel, first, last, together, ring, columns),
            out_shape=out_shape,
            in_specs=[VMEM] * 3 + extra_specs + [VMEM] * len(arrived),
            out_specs=[HBM if last else VMEM] * len(out_shape),
            scratch_shapes=[
                pltpu.VMEM((count, layers + 2, breadth + 2 * ROWS, LANES), jnp.float32),
                pltpu.VMEM((sizes.groups, ROWS, LANES), jnp.float32),
            ]
            + leaving * last,
            cost_estimate=cost(8_000_000, 3_000_000),
            compiler_params=PARAMS,
        )(fields, solute, mixed, *extra, *arrived)
        fields, solute = outs[:2]
        outs = list(outs[2:])
        if first or last:
            heat = outs.pop(0)
        if not last:
            mixed, faces = outs[0], outs[1:]
            arrived = exchange(faces)
    return (fields, solute, heat)


def solution(mesh):
    in_specs = (
        P(None, "gz", "gx", "gy"),
        P("gz", "gx", "gy"),
        P("gz", "gx", "gy", None, None),
        P("gz", "gx", "gy", None),
        P("gz", "gx", "gy", None),
        P("gz", "gx", "gy", None, None),
    )
    out_specs = (P(None, "gz", "gx", "gy"), P("gz", "gx", "gy"), P("gz", "gx", "gy"))

    return jax.shard_map(body, mesh=mesh, in_specs=in_specs, out_specs=out_specs, check_vma=False)
```

```python
import functools

import jax
import jax.numpy as jnp
from jax import lax
from jax.experimental import pallas as pl
from jax.experimental.pallas import tpu as pltpu
from jax.sharding import PartitionSpec as P


NODES = 16
STEPS = 3
LANES = 128
ROWS = 8
FAR = 4096

VMEM = pl.BlockSpec(memory_space=pltpu.VMEM)
HBM = pl.BlockSpec(memory_space=pltpu.HBM)
SMEM = pl.BlockSpec(memory_space=pltpu.SMEM)

PARAMS = pltpu.CompilerParams(vmem_limit_bytes=12 * 1024 * 1024)


def log2(size):
    assert size & (size - 1) == 0
    return size.bit_length() - 1


def half_up(start):
    return (start + (start & 1)) >> 1


def route_kernel(ring, capacity, table, *refs):
    lists, parity, picks = refs[:ring], refs[ring], refs[ring + 1]
    entries = table.shape[-1]
    me = lax.axis_index("gz")
    owners = [table[1, 0, e] for e in range(entries)]
    for axis in range(2):
        odd = jnp.int32(0)
        for e in range(entries):
            odd = odd | jnp.where(owners[e] >= 0, table[2 + axis, 0, e] & 1, 0)
        parity[axis] = odd
    for distance in range(ring):
        target = lax.rem(me + distance, ring)
        found = jnp.int32(0)
        for e in range(entries):
            picks[found] = e
            found = found + (owners[e] == target).astype(jnp.int32)
        for c in range(capacity):
            held = c < found
            e = jnp.where(held, picks[c], 0)
            lists[distance][4 * c] = jnp.maximum(table[0, 0, e], 0)
            for axis in range(3):
                lists[distance][4 * c + 1 + axis] = jnp.where(held, table[2 + axis, 0, e], FAR)


def project_kernel(ring, capacity, columns, *refs):
    lists, thermal, outs, both = refs[:ring], refs[ring], refs[ring + 1 : -1], refs[-1]
    tall = 2 * ROWS
    shape = (2 * tall, LANES)
    row = lax.broadcasted_iota(jnp.int32, shape, 0)
    node_x = ((row & 1) << 3) + (lax.broadcasted_iota(jnp.int32, shape, 1) >> log2(NODES))
    plane = lax.broadcasted_iota(jnp.int32, (tall, LANES), 0) >> 1
    cell_y = lax.broadcasted_iota(jnp.int32, (NODES, LANES), 1)
    node_y = 2 * lax.broadcasted_iota(jnp.int32, (NODES, LANES), 0)
    for distance in range(ring):
        total = None
        for c in range(capacity):
            slot, z, x, y = (lists[distance][4 * c + i] for i in range(4))
            rise = half_up(z)
            planes = pltpu.roll(thermal[slot], (2 * rise) & (2 * NODES - 1), 0)[:tall]
            planes = jnp.where((plane >= rise) & (plane < rise + NODES), planes, 0.0)
            coarse = planes.astype(jnp.bfloat16).astype(jnp.float32)
            pair = jnp.concatenate([coarse, planes - coarse], axis=0).astype(jnp.bfloat16)
            shift = half_up(x)
            spread = jnp.concatenate(
                [pair * (node_x == j - shift).astype(jnp.float32).astype(jnp.bfloat16) for j in range(columns)],
                axis=0,
            )
            distance_y = (cell_y - y - node_y).astype(jnp.float32)
            hat = jnp.maximum(0.0, 1.0 - 0.5 * jnp.abs(distance_y)).astype(jnp.bfloat16)
            weight = jnp.concatenate([hat] * (LANES // NODES), axis=0)
            part = jnp.dot(spread, weight, preferred_element_type=jnp.float32)
            total = part if total is None else total + part
        total = total.reshape(columns, 2, tall, LANES)
        both[distance] = (total[:, 0] + total[:, 1]).reshape(columns * tall, LANES)
        even, odd = (both[distance, pl.ds(i, columns * ROWS, stride=2), :] for i in range(2))
        outs[distance][...] = (even + odd).reshape(columns, ROWS, LANES)


def is_odd(axis):
    return (lax.axis_index(axis) & 1) == 1


class Faces:
    def __init__(self, count, layers, breadth, x_low, x_high, y_out, z_first, z_second):
        self.count, self.layers, self.breadth = count, layers, breadth
        self.halves = breadth // ROWS
        self.width = 2 * layers * self.halves
        self.per = LANES // self.width
        self.groups = -(-count // self.per)
        self.x_low, self.x_high, self.y_out = x_low, x_high, y_out
        self.z_first, self.z_second = z_first, z_second

    def lane(self, f, z, half):
        return (f % self.per) * self.width + 2 * (z * self.halves + half)

    def pack(self, fields, extra):
        lanes = lax.broadcasted_iota(jnp.int32, (ROWS, LANES), 1)
        odd = is_odd("gz")
        packed = [None] * self.groups
        for f in range(self.count):
            source = fields.at[f] if f < self.count - 1 else extra
            flat = source.reshape(self.layers * self.breadth, LANES)
            self.x_low[f] = flat[pl.ds(0, self.layers, stride=self.breadth), :]
            self.x_high[f] = flat[pl.ds(self.breadth - 1, self.layers, stride=self.breadth), :]
            low, high = source[0], source[self.layers - 1]
            self.z_first[f] = jnp.where(odd, low, high)
            self.z_second[f] = jnp.where(odd, high, low)
            group = f // self.per
            for z in range(self.layers):
                for half in range(self.halves):
                    k = self.lane(f, z, half)
                    turned = pltpu.roll(source[z, half * ROWS : (half + 1) * ROWS, :], k + 1, 1)
                    known = packed[group]
                    packed[group] = turned if known is None else jnp.where(lanes >> 1 == k >> 1, turned, known)
        for group in range(self.groups):
            self.y_out[group] = packed[group]


def split_x(refs, together):
    if together:
        return (refs[0].at[0], refs[0].at[1]), refs[1:]
    return (refs[0], refs[1]), refs[2:]


def pack_kernel(together, grains, solute, mixed, *rest):
    (x_low, x_high), (y_out, z_first, z_second) = split_x(rest, together)
    orders, layers, breadth, _ = grains.shape
    for z in range(layers):
        squares = None
        for f in range(orders):
            cells = grains[f, z]
            squares = cells * cells if squares is None else squares + cells * cells
        mixed[z] = solute[z] - 0.5 * squares
    Faces(orders + 1, layers, breadth, x_low, x_high, y_out, z_first, z_second).pack(grains, mixed)


def finish_kernel(ring, columns, *refs):
    parts, parity, heat = refs[:ring], refs[ring], refs[ring + 1]
    layers, breadth, _ = heat.shape
    lattice = parts[0][...]
    for part in parts[1:]:
        lattice = lattice + part[...]
    coarse = lattice.astype(jnp.bfloat16).astype(jnp.float32)
    pair = jnp.concatenate([coarse, lattice - coarse], axis=1)
    pair = pair.reshape(columns * 2 * ROWS, LANES).astype(jnp.bfloat16)
    shape = (layers * breadth, columns * 2 * ROWS)
    cell = lax.broadcasted_iota(jnp.int32, shape, 0)
    node = lax.broadcasted_iota(jnp.int32, shape, 1)

    def hat(position, index, odd):
        gap = (position + odd - 2 * index).astype(jnp.float32)
        return jnp.maximum(0.0, 1.0 - 0.5 * jnp.abs(gap))

    weight = hat(cell >> log2(breadth), node & (ROWS - 1), parity[0]) * hat(
        cell & (breadth - 1), node >> log2(2 * ROWS), parity[1]
    )
    warm = jnp.dot(weight.astype(jnp.bfloat16), pair, preferred_element_type=jnp.float32)
    heat[...] = warm.reshape(layers, breadth, LANES)


def inner_kernel(fields, solute, mixed, heat, fields_out, solute_out, wide):
    orders, layers, breadth, _ = fields.shape
    lanes = lax.broadcasted_iota(jnp.int32, (breadth, LANES), 1)
    nothing = jnp.zeros((layers, LANES), jnp.float32)
    for f in range(orders + 1):
        source = fields.at[f] if f < orders else mixed
        wide[f, :, ROWS : ROWS + breadth, :] = source[...]
        wide[f, :, ROWS - 1, :] = nothing
        wide[f, :, ROWS + breadth, :] = nothing

    def around(f, z, cells):
        total = wide[f, z, ROWS - 1 : ROWS - 1 + breadth, :] + wide[f, z, ROWS + 1 : ROWS + 1 + breadth, :]
        source = fields.at[f] if f < orders else mixed
        if z > 0:
            total = total + source[z - 1]
        if z < layers - 1:
            total = total + source[z + 1]
        below = jnp.where(lanes == 0, 0.0, pltpu.roll(cells, 1, 1))
        above = jnp.where(lanes == LANES - 1, 0.0, pltpu.roll(cells, LANES - 1, 1))
        return total + (below + above)

    for z in range(layers):
        squares = None
        for f in range(orders):
            cells = fields[f, z]
            squares = cells * cells if squares is None else squares + cells * cells
        here, level = solute[z], mixed[z]
        pull = 0.04 - 0.1 * squares
        drive = 6.0 * (1.0 - heat[z] - 0.5 * here)
        solute_out[z] = here + 0.15 * (around(orders, z, level) - 6.0 * level)
        for f in range(orders):
            cells = fields[f, z]
            well = cells * (1.0 - cells)
            fields_out[f, z] = (
                0.16 * around(f, z, cells)
                + cells * (pull + 0.1 * (cells * cells))
                + well * (drive * well + (0.4 * cells - 0.2))
            )


def outer_kernel(last, together, *refs):
    refs = list(refs)
    take = lambda n: [refs.pop(0) for _ in range(n)]
    fields, solute = take(2)
    heat = take(1)[0] if last else None
    if together:
        (arrived,) = take(1)
        x_low, x_high = arrived.at[1], arrived.at[0]
    else:
        x_low, x_high = take(2)
    y_first, y_second, z_first, z_second = take(4)
    orders, layers, breadth, _ = fields.shape
    if last:
        far_fields, far_solute, far_heat, solute_out, fields_out, leaving = refs
        faces = Faces(orders + 1, layers, breadth, None, None, None, None, None)
    else:
        fields_out, solute_out, mixed_out = take(3)
        (out_low, out_high), rest = split_x(refs, together)
        faces = Faces(orders + 1, layers, breadth, out_low, out_high, *rest)
    lanes = lax.broadcasted_iota(jnp.int32, (ROWS, LANES), 1)
    ends = (lanes == 0) | (lanes == LANES - 1)
    odd_z, odd_y = is_odd("gz"), is_odd("gy")
    copies = []
    if last:
        copies.append(pltpu.make_async_copy(heat, far_heat, leaving.at[orders + 1]))
        copies[-1].start()
    turned = []
    for group in range(faces.groups):
        first, second = y_first[group], y_second[group]
        below, above = jnp.where(odd_y, first, second), jnp.where(odd_y, second, first)
        turned.append(jnp.where((lanes & 1) == 1, pltpu.roll(below, 1, 1), pltpu.roll(above, LANES - 1, 1)))
    for f in range(orders + 1):
        source, target = (fields.at[f], fields_out.at[f]) if f < orders else (solute, solute_out)
        rate = 0.16 if f < orders else 0.15
        for z in range(layers):
            sides = []
            for half in range(faces.halves):
                k = faces.lane(f, z, half)
                beyond = pltpu.roll(turned[f // faces.per], LANES - 1 - k, 1)
                sides.append(jnp.where(ends, beyond, 0.0))
            total = jnp.concatenate(sides, axis=0)
            if z == 0:
                total = total + jnp.where(odd_z, z_first[f], z_second[f])
            if z == layers - 1:
                total = total + jnp.where(odd_z, z_second[f], z_first[f])
            target[z] = source[z] + rate * total
        flat = target.reshape(layers * breadth, LANES)
        for row, beyond in ((0, x_low), (breadth - 1, x_high)):
            edge = pl.ds(row, layers, stride=breadth)
            flat[edge, :] = flat[edge, :] + rate * beyond[f]
        if last:
            where_to = far_fields.at[f] if f < orders else far_solute
            copies.append(pltpu.make_async_copy(target, where_to, leaving.at[f]))
            copies[-1].start()
    if last:
        for copy in copies:
            copy.wait()
        return
    for z in range(layers):
        squares = None
        for f in range(orders):
            value = fields_out[f, z]
            squares = value * value if squares is None else squares + value * value
        mixed_out[z] = solute_out[z] - 0.5 * squares
    faces.pack(fields_out, mixed_out)


def shape_of(*dims, dtype=jnp.float32):
    return jax.ShapeDtypeStruct(dims, dtype)


def cost(flops, moved):
    return pl.CostEstimate(flops=flops, bytes_accessed=moved, transcendentals=0)


def around_ring(axis, distance):
    count = lax.axis_size(axis)
    return [(i, (i + distance) % count) for i in range(count)]


def send(value, axis, pairs):
    return lax.ppermute(value, axis, pairs)


def swaps(axis, closed):
    count = lax.axis_size(axis)
    assert count % 2 == 0
    first = [(i, i ^ 1) for i in range(count)]
    second = [(i, (i + 1 if i % 2 else i - 1) % count) for i in range(count)]
    if not closed:
        second = [(0, 0)] + second[1:-1] + [(count - 1, count - 1)]
    return first, second


def body(grains, solute, thermal, block_slot, block_owner, block_offset):
    ring = lax.axis_size("gz")
    across = lax.axis_size("gx")
    together = across == 2
    orders, layers, breadth, length = grains.shape
    slots = thermal.shape[3]
    capacity = slots // ring
    columns = breadth // 2 + 1
    count = orders + 1
    entries = block_slot.shape[-1]
    assert length == LANES and breadth % ROWS == 0 and layers // 2 + 1 <= ROWS

    table = jnp.concatenate(
        [array.reshape(-1, 1, entries) for array in (block_slot, block_owner, block_offset)], axis=0
    )
    routed = pl.pallas_call(
        functools.partial(route_kernel, ring, capacity),
        out_shape=[shape_of(4 * capacity, dtype=jnp.int32)] * ring + [shape_of(2, dtype=jnp.int32)],
        in_specs=[SMEM],
        out_specs=[SMEM] * (ring + 1),
        scratch_shapes=[pltpu.SMEM((entries + 1,), jnp.int32)],
        compiler_params=PARAMS,
        cost_estimate=cost(1_000_000_000, 1_000),
        name="route",
    )(table)
    asked, parity = routed[:ring], routed[ring]
    asked = [asked[0]] + [send(asked[d], "gz", around_ring("gz", d)) for d in range(1, ring)]

    sizes = Faces(count, layers, breadth, None, None, None, None, None)
    face_x = [shape_of(2, count, layers, length)] if together else [shape_of(count, layers, length)] * 2
    face_shapes = face_x + [shape_of(sizes.groups, ROWS, LANES)] + [shape_of(count, breadth, length)] * 2
    tile = shape_of(layers, breadth, length)

    packed = pl.pallas_call(
        functools.partial(pack_kernel, together),
        out_shape=[tile] + face_shapes,
        in_specs=[VMEM] * 2,
        out_specs=[VMEM] * (1 + len(face_shapes)),
        cost_estimate=cost(400_000_000, 2_000_000),
        compiler_params=PARAMS,
        name="pack",
    )(grains, solute)

    def exchange(faces):
        y_out, z_first, z_second = faces[-3:]
        y_swaps, z_swaps = swaps("gy", True), swaps("gz", False)
        if together:
            moved = [send(faces[0], "gx", around_ring("gx", 1))]
        else:
            moved = [send(faces[1], "gx", around_ring("gx", 1)), send(faces[0], "gx", around_ring("gx", -1))]
        return moved + [
            send(y_out, "gy", y_swaps[0]),
            send(y_out, "gy", y_swaps[1]),
            send(z_first, "gz", z_swaps[0]),
            send(z_second, "gz", z_swaps[1]),
        ]

    mixed, faces = packed[0], packed[1:]
    arrived = exchange(faces)

    nodes = thermal.reshape(slots, NODES**3 // LANES, LANES)
    assert NODES**2 == 2 * LANES
    lattice = shape_of(columns, ROWS, length)
    parts = pl.pallas_call(
        functools.partial(project_kernel, ring, capacity, columns),
        out_shape=[lattice] * ring,
        in_specs=[SMEM] * ring + [VMEM],
        out_specs=[VMEM] * ring,
        scratch_shapes=[pltpu.VMEM((ring, columns * 2 * ROWS, LANES), jnp.float32)],
        cost_estimate=cost(4_000_000, 1_000_000),
        compiler_params=PARAMS,
        name="project",
    )(*asked, nodes)
    parts = [parts[0]] + [send(parts[d], "gz", around_ring("gz", -d)) for d in range(1, ring)]

    heat = pl.pallas_call(
        functools.partial(finish_kernel, ring, columns),
        out_shape=tile,
        in_specs=[VMEM] * ring + [SMEM],
        out_specs=VMEM,
        compiler_params=PARAMS,
        cost_estimate=cost(10_000_000, 1_000_000),
        name="finish0",
    )(*parts, parity)

    fields = grains
    for turn in range(STEPS):
        last = turn == STEPS - 1
        inner = pl.pallas_call(
            inner_kernel,
            out_shape=[shape_of(*grains.shape), tile],
            in_specs=[VMEM] * 4,
            out_specs=[VMEM] * 2,
            scratch_shapes=[pltpu.VMEM((count, layers, breadth + 2 * ROWS, LANES), jnp.float32)],
            compiler_params=PARAMS,
            cost_estimate=cost(8_000_000, 3_000_000),
        )(fields, solute, mixed, heat)
        out_shape = [shape_of(*grains.shape), tile, tile] + ([] if last else face_shapes)
        leaving = [
            pltpu.VMEM((layers, breadth, length), jnp.float32),
            pltpu.VMEM(grains.shape, jnp.float32),
            pltpu.SemaphoreType.DMA((count + 1,)),
        ]
        outs = pl.pallas_call(
            functools.partial(outer_kernel, last, together),
            out_shape=out_shape,
            in_specs=[VMEM] * (2 + last + len(arrived)),
            out_specs=[HBM if last else VMEM] * len(out_shape),
            scratch_shapes=leaving * last,
            compiler_params=PARAMS,
            cost_estimate=cost(8_000_000, 3_000_000),
        )(*inner, *[heat] * last, *arrived)
        fields, solute = outs[:2]
        if last:
            heat = outs[2]
        else:
            mixed, faces = outs[2], outs[3:]
            arrived = exchange(faces)
    return (fields, solute, heat)


def solution(mesh):
    in_specs = (
        P(None, "gz", "gx", "gy"),
        P("gz", "gx", "gy"),
        P("gz", "gx", "gy", None, None),
        P("gz", "gx", "gy", None),
        P("gz", "gx", "gy", None),
        P("gz", "gx", "gy", None, None),
    )
    out_specs = (P(None, "gz", "gx", "gy"), P("gz", "gx", "gy"), P("gz", "gx", "gy"))

    return jax.shard_map(body, mesh=mesh, in_specs=in_specs, out_specs=out_specs, check_vma=False)
```
